32 devices in a mesh: data: 32 (over z, y, x, core).
Axes of the slice: x: 2, y: 2, z: 4, core: 2. Of those that a mesh axis runs over, the one named last changes fastest.
Arguments:
- act_in: bfloat16 [131072, 960], P('data')
- grad_out: bfloat16 [131072, 960], P('data')
- w_up1: bfloat16 [960, 2560], replicated
- w_down1: bfloat16 [2560, 960], replicated
- w_up2: bfloat16 [960, 2560], replicated
- w_down2: bfloat16 [2560, 960], replicated
- master_up1: float32 [960, 2560], P('data')
- master_down1: float32 [2560, 960], P('data')
- master_up2: float32 [960, 2560], P('data')
- master_down2: float32 [2560, 960], P('data')
- mom_up1: float32 [960, 2560], P('data')
- mom_down1: float32 [2560, 960], P('data')
- mom_up2: float32 [960, 2560], P('data')
- mom_down2: float32 [2560, 960], P('data')
- vel_up1: float32 [960, 2560], P('data')
- vel_down1: float32 [2560, 960], P('data')
- vel_up2: float32 [960, 2560], P('data')
- vel_down2: float32 [2560, 960], P('data')
- learn_rate: float32 [], replicated
- clip_norm: float32 [], replicated
Outputs:
- output 1: bfloat16 [960, 2560], replicated
- output 2: bfloat16 [2560, 960], replicated
- output 3: bfloat16 [960, 2560], replicated
- output 4: bfloat16 [2560, 960], replicated
- output 5: float32 [960, 2560], P('data')
- output 6: float32 [2560, 960], P('data')
- output 7: float32 [960, 2560], P('data')
- output 8: float32 [2560, 960], P('data')
- output 9: float32 [960, 2560], P('data')
- output 10: float32 [2560, 960], P('data')
- output 11: float32 [960, 2560], P('data')
- output 12: float32 [2560, 960], P('data')
- output 13: float32 [960, 2560], P('data')
- output 14: float32 [2560, 960], P('data')
- output 15: float32 [960, 2560], P('data')
- output 16: float32 [2560, 960], P('data')
- output 17: float32 [], replicated
All inputs are finite; a program needn't handle non-finite values.
Results may differ from the reference program's by a relative error of at most 0.0117184.
Values are sent between devices in bfloat16 or wider.
A program may use at most 1 GiB of HBM per device.

```python
import math
import jax
import jax.numpy as jnp
from jax import lax

D = 960
FF = 2560
ROWS = 131072
GROUP = 32
STEP = 20
SAMPLE = 256

BETA_ONE = 0.9
BETA_TWO = 0.95
EPSILON = 1e-8
NORM_EPS = 1e-6
CORR_ONE = 1.0 - BETA_ONE ** STEP
CORR_TWO = 1.0 - BETA_TWO ** STEP
ROOT_HALF = math.sqrt(0.5)
INV_ROOT_TAU = 1.0 / math.sqrt(2.0 * math.pi)
LAYER_GAINS = (1.0, 1.5, 1.0, 2.0)
LAYER_NAMES = ("up1", "down1", "up2", "down2")


def gelu_pair(pre):
    normal_cdf = 0.5 * (1.0 + lax.erf(pre * ROOT_HALF))
    density = jnp.exp(-0.5 * pre * pre) * INV_ROOT_TAU
    return pre * normal_cdf, normal_cdf + pre * density


def fwd_bwd(rows_in, rows_grad, w_up1, w_down1, w_up2, w_down2):
    pre_up1 = jnp.dot(rows_in, w_up1, preferred_element_type=jnp.float32)
    gel_up1, der_up1 = gelu_pair(pre_up1)
    act_up1 = gel_up1.astype(jnp.bfloat16)
    mid_act = jnp.dot(act_up1, w_down1, preferred_element_type=jnp.float32).astype(jnp.bfloat16)
    pre_up2 = jnp.dot(mid_act, w_up2, preferred_element_type=jnp.float32)
    gel_up2, der_up2 = gelu_pair(pre_up2)
    act_up2 = gel_up2.astype(jnp.bfloat16)
    grad_act2 = jnp.dot(rows_grad, w_down2.T, preferred_element_type=jnp.float32).astype(jnp.bfloat16)
    grad_pre2 = (grad_act2.astype(jnp.float32) * der_up2).astype(jnp.bfloat16)
    grad_mid = jnp.dot(grad_pre2, w_up2.T, preferred_element_type=jnp.float32).astype(jnp.bfloat16)
    grad_act1 = jnp.dot(grad_mid, w_down1.T, preferred_element_type=jnp.float32).astype(jnp.bfloat16)
    grad_pre1 = (grad_act1.astype(jnp.float32) * der_up1).astype(jnp.bfloat16)
    return ((act_up2, rows_grad), (mid_act, grad_pre2), (act_up1, grad_mid), (rows_in, grad_pre1))


def adam_step(grad_rows, master_old, mom_old, vel_old, clip_scale, learn_rate):
    scaled = clip_scale * grad_rows
    mom_new = BETA_ONE * mom_old + (1.0 - BETA_ONE) * scaled
    vel_new = BETA_TWO * vel_old + (1.0 - BETA_TWO) * scaled * scaled
    master_new = master_old - learn_rate * (mom_new / CORR_ONE) / (jnp.sqrt(vel_new / CORR_TWO) + EPSILON)
    return master_new.astype(jnp.bfloat16), master_new, mom_new, vel_new


def norm_estimate(act_in, grad_out, weights):
    stride = ROWS // SAMPLE
    grad_pairs = fwd_bwd(act_in[::stride], grad_out[::stride], weights[0], weights[1], weights[2], weights[3])
    row_total = 0.0
    for layer_in, layer_delta in grad_pairs:
        in_sq = jnp.sum(jnp.square(layer_in.astype(jnp.float32)), axis=1)
        delta_sq = jnp.sum(jnp.square(layer_delta.astype(jnp.float32)), axis=1)
        row_total = row_total + jnp.sum(in_sq * delta_sq)
    return jnp.sqrt(row_total * stride) / GROUP


def setup_inputs(seed: int = 0) -> dict:
    key_list = jax.random.split(jax.random.key(seed), 20)
    act_in = jax.random.normal(key_list[0], (ROWS, D), jnp.float32).astype(jnp.bfloat16)
    grad_scale = 2.0 * GROUP / math.sqrt(ROWS * D * FF)
    grad_out = (grad_scale * jax.random.normal(key_list[1], (ROWS, D), jnp.float32)).astype(jnp.bfloat16)
    shapes = ((D, FF), (FF, D), (D, FF), (FF, D))
    weights = []
    masters = []
    for layer_idx in range(4):
        init_scale = LAYER_GAINS[layer_idx] / math.sqrt(shapes[layer_idx][0])
        weight = init_scale * jax.random.normal(key_list[2 + layer_idx], shapes[layer_idx], jnp.float32)
        weights.append(weight.astype(jnp.bfloat16))
        masters.append(weight + 0.01 * init_scale * jax.random.normal(key_list[6 + layer_idx], shapes[layer_idx], jnp.float32))
    clip_norm = norm_estimate(act_in, grad_out, weights) * jax.random.uniform(key_list[10], (), jnp.float32, 0.3, 0.6)
    unit_size = clip_norm / math.sqrt(4 * D * FF)
    inputs = {"act_in": act_in, "grad_out": grad_out}
    for layer_idx in range(4):
        inputs["w_" + LAYER_NAMES[layer_idx]] = weights[layer_idx]
    for layer_idx in range(4):
        inputs["master_" + LAYER_NAMES[layer_idx]] = masters[layer_idx]
    for layer_idx in range(4):
        inputs["mom_" + LAYER_NAMES[layer_idx]] = 0.1 * unit_size * jax.random.normal(key_list[11 + layer_idx], shapes[layer_idx], jnp.float32)
    for layer_idx in range(4):
        inputs["vel_" + LAYER_NAMES[layer_idx]] = 0.05 * unit_size * unit_size * jax.random.uniform(key_list[15 + layer_idx], shapes[layer_idx], jnp.float32, 0.5, 1.5)
    inputs["learn_rate"] = 0.5 / math.sqrt(D) * jax.random.uniform(key_list[19], (), jnp.float32, 0.2, 1.0)
    inputs["clip_norm"] = clip_norm
    return inputs


def reference(act_in, grad_out, w_up1, w_down1, w_up2, w_down2, master_up1, master_down1, master_up2, master_down2, mom_up1, mom_down1, mom_up2, mom_down2, vel_up1, vel_down1, vel_up2, vel_down2, learn_rate, clip_norm):
    rows_dev = ROWS // GROUP
    dev_in = act_in.reshape(GROUP, rows_dev, D)
    dev_grad = grad_out.reshape(GROUP, rows_dev, D)

    def accumulate(carry, block):
        grad_pairs = fwd_bwd(block[0], block[1], w_up1, w_down1, w_up2, w_down2)
        summed = tuple(carry[layer_idx] + jnp.dot(grad_pairs[layer_idx][0].T, grad_pairs[layer_idx][1], preferred_element_type=jnp.float32) for layer_idx in range(4))
        return summed, None

    start_sums = (jnp.zeros((FF, D), jnp.float32), jnp.zeros((D, FF), jnp.float32), jnp.zeros((FF, D), jnp.float32), jnp.zeros((D, FF), jnp.float32))
    totals = lax.scan(accumulate, start_sums, (dev_in, dev_grad))[0]
    grad_list = [totals[3] / GROUP, totals[2] / GROUP, totals[1] / GROUP, totals[0] / GROUP]
    grad_norm = jnp.sqrt(sum(jnp.sum(grad_rows * grad_rows) for grad_rows in grad_list))
    clip_scale = jnp.minimum(1.0, clip_norm / (grad_norm + NORM_EPS))
    state_up1 = adam_step(grad_list[0], master_up1, mom_up1, vel_up1, clip_scale, learn_rate)
    state_down1 = adam_step(grad_list[1], master_down1, mom_down1, vel_down1, clip_scale, learn_rate)
    state_up2 = adam_step(grad_list[2], master_up2, mom_up2, vel_up2, clip_scale, learn_rate)
    state_down2 = adam_step(grad_list[3], master_down2, mom_down2, vel_down2, clip_scale, learn_rate)
    return (state_up1[0], state_down1[0], state_up2[0], state_down2[0], state_up1[1], state_down1[1], state_up2[1], state_down2[1], state_up1[2], state_down1[2], state_up2[2], state_down2[2], state_up1[3], state_down1[3], state_up2[3], state_down2[3], grad_norm)
```

```python
import functools
import math
import jax
import jax.numpy as jnp
from jax import lax
from jax.experimental import pallas as pl
from jax.experimental.pallas import tpu as pltpu
from jax.sharding import PartitionSpec as P

STEP = 20
BETA_ONE = 0.9
BETA_TWO = 0.95
EPSILON = 1e-8
NORM_EPS = 1e-6
CORR_ONE = 1.0 - BETA_ONE ** STEP
CORR_TWO = 1.0 - BETA_TWO ** STEP
ROOT_HALF = math.sqrt(0.5)
INV_ROOT_TAU = 1.0 / math.sqrt(2.0 * math.pi)
D, FF, DEVS = 960, 2560, 32
UP, DOWN = D // DEVS, FF // DEVS

ORDERS = ((1, 2, 4, 8, 16), (1, 4, 2, 8, 16), (1, 8, 4, 2, 16))
SIZES = (16, 8, 4, 2, 1)
BASES = (0, 16, 24, 28, 30)
KINDS = ("down", "up", "down", "up")
CHUNKS = 10
PARTS = 5


def mat_nt(left, right):
    return lax.dot_general(left, right, (((1,), (1,)), ((), ())), preferred_element_type=jnp.float32)


def mat_tn(left, right):
    return lax.dot_general(left, right, (((0,), (0,)), ((), ())), preferred_element_type=jnp.float32)


def gelu_pair(pre):
    normal_cdf = 0.5 * (1.0 + lax.erf(pre * ROOT_HALF))
    density = jnp.exp(-0.5 * pre * pre) * INV_ROOT_TAU
    return pre * normal_cdf, normal_cdf + pre * density


def fwd_bwd(rows_in, rows_grad, w_up1, w_down1, w_up2, w_down2):
    pre_up1 = jnp.dot(rows_in, w_up1, preferred_element_type=jnp.float32)
    gel_up1, der_up1 = gelu_pair(pre_up1)
    act_up1 = gel_up1.astype(jnp.bfloat16)
    mid_act = jnp.dot(act_up1, w_down1, preferred_element_type=jnp.float32).astype(jnp.bfloat16)
    pre_up2 = jnp.dot(mid_act, w_up2, preferred_element_type=jnp.float32)
    gel_up2, der_up2 = gelu_pair(pre_up2)
    act_up2 = gel_up2.astype(jnp.bfloat16)
    grad_act2 = mat_nt(rows_grad, w_down2).astype(jnp.bfloat16)
    grad_pre2 = (grad_act2.astype(jnp.float32) * der_up2).astype(jnp.bfloat16)
    grad_mid = mat_nt(grad_pre2, w_up2).astype(jnp.bfloat16)
    grad_act1 = mat_nt(grad_mid, w_down1).astype(jnp.bfloat16)
    grad_pre1 = (grad_act1.astype(jnp.float32) * der_up1).astype(jnp.bfloat16)
    return ((act_up2, rows_grad), (mid_act, grad_pre2), (act_up1, grad_mid), (rows_in, grad_pre1))


def position(dev, order):
    return sum(((dev // bit) % 2) * size for bit, size in zip(order, SIZES))


class Route:
    def __init__(self):
        self.me = lax.axis_index("data")
        self.bits = {bit: (self.me // bit) % 2 for bit in (1, 2, 4, 8, 16)}
        self.peers = {bit: self.me + bit * (1 - 2 * self.bits[bit]) for bit in (1, 2, 4, 8, 16)}

    def start_of(self, order, stage):
        return sum((self.bits[order[k]] * SIZES[k] for k in range(stage)), 0)


def barrier_with(peers):
    sem = pltpu.get_barrier_semaphore()
    for peer in peers:
        pl.semaphore_signal(sem, inc=1, device_id=(peer,), device_id_type=pl.DeviceIdType.MESH)
    pl.semaphore_wait(sem, len(peers))


def stream_chunk(stream, i):
    per = (4, 3, 3)[stream]
    return (i // per) * CHUNKS + stream + 3 * (i % per)


def reduce_tick(route, t, gbuf, recv, ssem, rsem, gsh):
    for stream, order in enumerate(ORDERS):
        count = (16, 12, 12)[stream]
        for stage in (5, 4, 3, 2, 1, 0):
            i = t - stage

            @pl.when((i >= 0) & (i < count))
            def _(stream=stream, order=order, stage=stage, i=i):
                c = stream_chunk(stream, i)
                slot = lax.rem(i, 2)

                def copy(k):
                    bit, n = order[k], SIZES[k]
                    away = route.start_of(order, k) + (1 - route.bits[bit]) * n
                    return pltpu.make_async_remote_copy(
                        src_ref=gbuf.at[c, pl.ds(away, n)],
                        dst_ref=recv.at[stream, slot, pl.ds(BASES[k], n)],
                        send_sem=ssem.at[stream, slot, k], recv_sem=rsem.at[stream, slot, k],
                        device_id=(route.peers[bit],), device_id_type=pl.DeviceIdType.MESH)

                if stage > 0:
                    last = stage - 1
                    copy(last).wait()
                    kept, n = route.start_of(order, stage), SIZES[last]
                    if stage < 5:
                        for b in range(n):
                            gbuf[c, kept + b] += recv[stream, slot, BASES[last] + b]
                    else:
                        gsh[c] = (gbuf[c, kept] + recv[stream, slot, BASES[last]]) * (1.0 / DEVS)
                if stage < 5:
                    copy(stage).start()


def repack_up(tile, gbuf, chunk, order):
    for dev in range(DEVS):
        pos = position(dev, order)
        for group in range(4):
            rows = min(8, UP - 8 * group)
            gbuf[chunk, pos, 0:rows, 256 * group:256 * (group + 1)] = tile[UP * dev + 8 * group:UP * dev + 8 * group + rows, :]
        gbuf[chunk, pos, 6:8, 768:1024] = jnp.zeros((2, 256), jnp.float32)


def reduce_kernel(g4, g3, g2, g1, gsh_out, norm_out, gbuf, recv, tile, gsh, sums, load_sem, tile_sem, ssem, rsem, nsend, nrecv, out_sem):
    route = Route()
    everyone = [lax.rem(route.me + k, DEVS) for k in range(1, DEVS)]
    barrier_with(everyone)

    def down_loads():
        for k, ref in ((0, g4), (2, g2)):
            for stream, order in enumerate(ORDERS):
                for j in range(stream, CHUNKS, 3):
                    for dev in range(DEVS):
                        yield pltpu.make_async_copy(ref.at[dev, pl.ds(8 * j, 8)], gbuf.at[10 * k + j, position(dev, order)], load_sem)

    for copy in down_loads():
        copy.start()

    for k, ref in ((1, g3), (3, g1)):
        def fetch(j, ref=ref):
            return pltpu.make_async_copy(ref.at[:, pl.ds(pl.multiple_of(256 * j, 256), 256)], tile.at[j % 2], tile_sem.at[j % 2])
        fetch(0).start()
        for j in range(CHUNKS):
            if j + 1 < CHUNKS:
                fetch(j + 1).start()
            fetch(j).wait()
            repack_up(tile.at[j % 2], gbuf, 10 * k + j, ORDERS[j % 3])
    for k in (0, 2):
        pltpu.make_async_copy(gbuf.at[pl.ds(10 * k, 10)], gbuf.at[pl.ds(10 * k, 10)], load_sem).wait()

    def tick(t, carry):
        reduce_tick(route, t, gbuf, recv, ssem, rsem, gsh)
        return carry
    lax.fori_loop(0, 16 + 5, tick, 0)

    out = pltpu.make_async_copy(gsh, gsh_out, out_sem)
    out.start()

    def square(c, acc):
        g = gsh[c]
        return acc + g * g
    acc = lax.fori_loop(0, 4 * CHUNKS, square, jnp.zeros((8, 1024), jnp.float32))
    part = acc[:, 0:128]
    for k in range(1, 8):
        part = part + acc[:, 128 * k:128 * (k + 1)]
    sums[route.me] = part
    def tell(peer):
        return pltpu.make_async_remote_copy(src_ref=sums.at[route.me], dst_ref=sums.at[route.me], send_sem=nsend, recv_sem=nrecv,
                                            device_id=(peer,), device_id_type=pl.DeviceIdType.MESH)
    for peer in everyone:
        tell(peer).start()
    everything = pltpu.make_async_copy(sums.at[pl.ds(0, DEVS - 1)], sums.at[pl.ds(0, DEVS - 1)], nrecv)
    everything.wait()
    pltpu.make_async_copy(sums.at[pl.ds(0, DEVS - 1)], sums.at[pl.ds(0, DEVS - 1)], nsend).wait()
    total = sums[0]
    for dev in range(1, DEVS):
        total = total + sums[dev]
    total = jnp.sum(jnp.sum(total, axis=0, keepdims=True), axis=1, keepdims=True)
    norm_out[...] = jnp.broadcast_to(jnp.sqrt(total), (8, 128))
    out.wait()


def adam(grad, mom, vel, master, scale, rate):
    scaled = scale * grad
    mom_new = BETA_ONE * mom + (1.0 - BETA_ONE) * scaled
    vel_new = BETA_TWO * vel + (1.0 - BETA_TWO) * scaled * scaled
    master_new = master - rate * (mom_new / CORR_ONE) / (jnp.sqrt(vel_new / CORR_TWO) + EPSILON)
    return master_new, mom_new, vel_new


def pieces(kind, j):
    if kind == "down":
        return [(8 * j, 8, 0, D, 0)]
    return [(8 * i, min(8, UP - 8 * i), 256 * j, 256, 256 * i) for i in range(4)]


def gather_kernel(gsh, norm, lr, clip, *refs):
    states = [refs[3 * k:3 * k + 3] for k in range(4)]
    up_out, down_out, up_buf, down_buf, fresh, ssem, rsem, out_sem = refs[12:]
    route = Route()
    peers = list(route.peers.values())
    barrier_with(peers)
    rate = lr[0]
    scale = jnp.minimum(1.0, clip[0] / (norm[0:1, 0:1] + NORM_EPS))
    fresh[...] = jnp.zeros((32, FF), jnp.float32)

    for k, kind in enumerate(KINDS):
        master, mom, vel = states[k]
        half = k // 2
        for j in range(CHUNKS):
            for row, rows, col, cols, lane in pieces(kind, j):
                at = (slice(row, row + rows), slice(col, col + cols))
                new = adam(gsh[10 * k + j, 0:rows, lane:lane + cols], mom[at], vel[at], master[at], scale, rate)[0]
                fresh[(row if kind == "up" else 8 * (j % 2)):(row if kind == "up" else 8 * (j % 2)) + rows, col:col + cols] = new
            if kind == "down" and j % 2 == 1:
                p = j // 2
                unit = 5 * k + p
                down_buf[PARTS * half + p, position(route.me, ORDERS[unit % 3])] = fresh[0:16, 0:1024].astype(jnp.bfloat16)
        if kind == "up":
            for p in range(PARTS):
                unit = 5 * k + p
                up_buf[PARTS * half + p, position(route.me, ORDERS[unit % 3])] = fresh[:, 512 * p:512 * (p + 1)].astype(jnp.bfloat16)

    def unit_ref(unit):
        k, p = unit // PARTS, unit % PARTS
        return (up_buf if KINDS[k] == "up" else down_buf).at[PARTS * (k // 2) + p]

    def out_copy(unit):
        k, p = unit // PARTS, unit % PARTS
        dst = (up_out if KINDS[k] == "up" else down_out).at[PARTS * (k // 2) + p]
        return pltpu.make_async_copy(unit_ref(unit), dst, out_sem)

    def copy(unit, stage):
        order = ORDERS[unit % 3]
        k = 4 - stage
        bit, n = order[k], SIZES[k]
        mine = route.start_of(order, k) + route.bits[bit] * n
        ref = unit_ref(unit).at[pl.ds(mine, n)]
        return pltpu.make_async_remote_copy(src_ref=ref, dst_ref=ref, send_sem=ssem.at[unit, stage], recv_sem=rsem.at[unit, stage],
                                            device_id=(route.peers[bit],), device_id_type=pl.DeviceIdType.MESH)

    for t in range(7 + 5):
        for stage in (5, 4, 3, 2, 1, 0):
            for stream in range(3):
                unit = 3 * (t - stage) + stream
                if not (t - stage >= 0 and unit < 4 * PARTS):
                    continue
                if stage > 0:
                    copy(unit, stage - 1).wait()
                if stage < 5:
                    copy(unit, stage).start()
                else:
                    out_copy(unit).start()
    for unit in range(4 * PARTS):
        out_copy(unit).wait()


def finish_kernel(up_ref, down_ref, gsh, norm, lr, clip, *refs):
    states = [refs[3 * k:3 * k + 3] for k in range(4)]
    new_up, new_down = refs[12:14]
    outs = [refs[14 + 3 * k:17 + 3 * k] for k in range(4)]
    wide, tall = refs[26:28]
    step = pl.program_id(0)

    @pl.when(step == 0)
    def _():
        rate = lr[0]
        scale = jnp.minimum(1.0, clip[0] / (norm[0:1, 0:1] + NORM_EPS))
        for k, kind in enumerate(KINDS):
            for j in range(CHUNKS):
                for row, rows, col, cols, lane in pieces(kind, j):
                    at = (slice(row, row + rows), slice(col, col + cols))
                    master, mom, vel = (r[at] for r in states[k])
                    news = adam(gsh[10 * k + j, 0:rows, lane:lane + cols], mom, vel, master, scale, rate)
                    for out, new in zip(outs[k], news):
                        out[at] = new

    half, p = step // PARTS, step % PARTS
    for stream, order in enumerate(ORDERS):
        @pl.when(lax.rem(5 * (2 * half + 1) + p, 3) == stream)
        def _(order=order):
            for dev in range(DEVS):
                wide[UP * dev:UP * (dev + 1), :] = up_ref[0, position(dev, order), 0:UP, :].astype(jnp.float32)
        @pl.when(lax.rem(5 * 2 * half + p, 3) == stream)
        def _(order=order):
            for dev in range(DEVS):
                tall[dev] = down_ref[0, position(dev, order), :, 0:D]
    new_up[0] = wide[...].astype(jnp.bfloat16)
    new_down[0] = tall[...]


def solution(mesh):
    rows_spec = P("data", None)
    full_spec = P(None, None)
    vmem = pl.BlockSpec(memory_space=pltpu.VMEM)
    smem = pl.BlockSpec(memory_space=pltpu.SMEM)
    hbm = pl.BlockSpec(memory_space=pl.ANY)
    f32, bf16 = jnp.float32, jnp.bfloat16
    dma = pltpu.SemaphoreType.DMA

    def shard_body(act_in, grad_out, w_up1, w_down1, w_up2, w_down2, master_up1, master_down1, master_up2, master_down2, mom_up1, mom_down1, mom_up2, mom_down2, vel_up1, vel_down1, vel_up2, vel_down2, learn_rate, clip_norm):
        grad_pairs = fwd_bwd(act_in, grad_out, w_up1, w_down1, w_up2, w_down2)
        local = [mat_tn(a, b) for a, b in grad_pairs]
        for k in (0, 2):
            local[k] = jnp.pad(local[k], ((0, 0), (0, 64))).reshape(DEVS, DOWN, 1024)
        gsh, norm = pl.pallas_call(
            reduce_kernel,
            out_shape=(jax.ShapeDtypeStruct((40, 8, 1024), f32), jax.ShapeDtypeStruct((8, 128), f32)),
            in_specs=[hbm] * 4, out_specs=(hbm, vmem),
            scratch_shapes=[
                pltpu.VMEM((40, 32, 8, 1024), f32), pltpu.VMEM((3, 2, 31, 8, 1024), f32), pltpu.VMEM((2, D, 256), f32),
                pltpu.VMEM((40, 8, 1024), f32), pltpu.VMEM((32, 8, 128), f32),
                dma, dma((2,)), dma((3, 2, 5)), dma((3, 2, 5)), dma, dma, dma],
            compiler_params=pltpu.CompilerParams(collective_id=0, has_side_effects=True, vmem_limit_bytes=64 * 1024 * 1024 - 65536),
            name="reduce",
        )(*local)
        states = [master_down2, mom_down2, vel_down2, master_up2, mom_up2, vel_up2, master_down1, mom_down1, vel_down1, master_up1, mom_up1, vel_up1]
        lr, clip = learn_rate.reshape(1), clip_norm.reshape(1)
        up_all, down_all = pl.pallas_call(
            gather_kernel,
            out_shape=(jax.ShapeDtypeStruct((10, 32, 32, 512), bf16), jax.ShapeDtypeStruct((10, 32, 16, 1024), bf16)),
            in_specs=[vmem, vmem, smem, smem] + [vmem] * 12, out_specs=(hbm, hbm),
            scratch_shapes=[
                pltpu.VMEM((10, 32, 32, 512), bf16), pltpu.VMEM((10, 32, 16, 1024), bf16), pltpu.VMEM((32, FF), f32),
                dma((20, 5)), dma((20, 5)), dma],
            compiler_params=pltpu.CompilerParams(collective_id=1, has_side_effects=True, vmem_limit_bytes=48 * 1024 * 1024),
            name="gather",
        )(gsh, norm, lr, clip, *states)
        whole = lambda shape: pl.BlockSpec(shape, lambda s: (0,) * len(shape))
        state_shapes = [(DOWN, D)] * 3 + [(UP, FF)] * 3 + [(DOWN, D)] * 3 + [(UP, FF)] * 3
        res = pl.pallas_call(
            finish_kernel,
            grid=(10,),
            out_shape=(jax.ShapeDtypeStruct((2, D, FF), bf16), jax.ShapeDtypeStruct((2, DEVS, DOWN, D), bf16)) + tuple(jax.ShapeDtypeStruct(s, f32) for s in state_shapes),
            in_specs=[pl.BlockSpec((1, 32, 32, 512), lambda s: (s, 0, 0, 0)), pl.BlockSpec((1, 32, 16, 1024), lambda s: (s, 0, 0, 0)),
                      whole((40, 8, 1024)), whole((8, 128)), smem, smem] + [whole(s) for s in state_shapes],
            out_specs=(pl.BlockSpec((1, D, 512), lambda s: (s // PARTS, 0, s % PARTS)), pl.BlockSpec((1, DEVS, 16, D), lambda s: (s // PARTS, 0, s % PARTS, 0))) + tuple(whole(s) for s in state_shapes),
            scratch_shapes=[pltpu.VMEM((D, 512), f32), pltpu.VMEM((DEVS, 16, D), bf16)],
            compiler_params=pltpu.CompilerParams(vmem_limit_bytes=48 * 1024 * 1024),
            name="finish",
        )(up_all, down_all, gsh, norm, lr, clip, *states)
        new_up, new_down = res[0], res[1].reshape(2, FF, D)
        st = [res[2 + 3 * k:5 + 3 * k] for k in range(4)]
        order = (3, 2, 1, 0)
        weights = (new_up[1], new_down[1], new_up[0], new_down[0])
        return weights + tuple(st[k][f] for f in range(3) for k in order) + (norm[0, 0],)

    in_specs = (rows_spec, rows_spec) + (full_spec,) * 4 + (rows_spec,) * 12 + (P(), P())
    out_specs = (full_spec,) * 4 + (rows_spec,) * 12 + (P(),)
    return jax.shard_map(shard_body, mesh=mesh, in_specs=in_specs, out_specs=out_specs, check_vma=False)
```
